512 devices in a mesh: ens: 64 (over y, z_lo, core), slab: 8 (over x, z_hi).
Axes of the slice: x: 4, y: 4, z: 16 (z_hi: 2, z_lo: 8; z = z_hi * 8 + z_lo), core: 2. Of those that a mesh axis runs over, the one named last changes fastest.
Arguments:
- displacement: float32 [192, 24, 24, 128], P('ens', 'slab'), parts along dimension 0, may hold values from -0.75 to 0.75
- velocity: float32 [192, 24, 24, 128], P('ens', 'slab'), parts along dimension 0, may hold values from -6 to 6
- bond_mask: int32 [512, 24, 24, 128], P('ens', 'slab'), parts along dimension 0, may hold values from 0 to 65535, as said below
- moduli: float32 [16, 2], replicated, may hold values from 16 to 64
- material: int32 [64], P('ens'), parts along dimension 0, may hold values from 0 to 15
Outputs:
- new_displacement: float32 [192, 24, 24, 128], P('ens', 'slab'), parts along dimension 0
- new_velocity: float32 [192, 24, 24, 128], P('ens', 'slab'), parts along dimension 0
- energy: float32 [64], P('ens'), parts along dimension 0
The draws below stay inside these ranges and needn't reach their ends.
There are 64 independent parts, one for each index of `ens`. The reference program is written for one: setup_inputs(seed, part) draws one part's arguments, and reference() takes and returns one part's arrays. A program takes and returns all parts, laid end to end along the dimension named above; an argument that names none is the same for every part. Nothing has to cross between parts.
Inputs may be any that keep to these rules, and one draw needn't show every extreme that they name: `bond_mask`: bit number k mod 16 of word k // 16 is 1 where the bond along offset o_k of the list O is intact and 0 where it is broken; the bond along o_k from a cell p and the bond along -o_k from p + o_k carry the same bit wherever both cells lie in the grid; bits 10 to 15 of word 7 are 0.
All inputs are finite; a program needn't handle non-finite values.
Results may differ from the reference program's by a relative error of at most 0.00002.
Values sent between devices are 32-bit elements; how exact they have to be, the bound alone decides.
A program may use at most 64 MiB of HBM per device.

```python
import math
import jax
import jax.numpy as jnp
from jax import lax

NY = 24
NZ = 128
WORDS = 8
MATS = 16
NX = 24


def upward_offsets():
    found = []
    for a in range(-3, 4):
        for b in range(-3, 4):
            for c in range(-3, 4):
                if a * a + b * b + c * c <= 9 and (a, b, c) > (0, 0, 0):
                    found.append((a, b, c))
    return found


def draw_velocity(key, part):
    position = jnp.arange(NX, dtype=jnp.float32) / max(NX - 1, 1)
    profile = 0.5 + position
    random_part = jax.random.truncated_normal(key, -4.0, 4.0, (3, NX, NY, NZ), jnp.float32)
    return random_part * profile[None, :, None, None]


def draw_bond_mask(key, part):
    packed = [jnp.zeros((NX, NY, NZ), jnp.int32) for number in range(WORDS)]
    upward = upward_offsets()
    count = len(upward)
    for k, (a, b, c) in enumerate(upward):
        intact = (jax.random.randint(jax.random.fold_in(key, k), (NX, NY, NZ), 0, 4) != 0).astype(jnp.int32)
        mirror = jnp.roll(intact, (a, b, c), axis=(0, 1, 2))
        packed[k // 16] = packed[k // 16] + intact * 2 ** (k % 16)
        packed[(k + count) // 16] = packed[(k + count) // 16] + mirror * 2 ** ((k + count) % 16)
    return jnp.stack(packed)


def block_levels(rng, dims, split, low, largest):
    def one(dim, shards_of):
        draws = jax.random.uniform(jax.random.fold_in(jax.random.fold_in(rng, 6), dim), (shards_of,), jnp.float32, low / len(split), largest / len(split))
        return jnp.repeat(jnp.exp(draws), dims[dim] // shards_of).reshape((-1,) + (1,) * (len(dims) - dim - 1))

    loudness = one(*split[0])
    for cut in split[1:]:
        loudness = loudness * one(*cut)
    return loudness


def noise(rng, dims, deviation, limit, pieces=(), kind=jnp.bfloat16):
    gain = block_levels(rng, dims, pieces, -0.22, 0.18) if pieces else 1.0
    drawn = jax.random.normal(rng, dims, jnp.float32) * deviation * gain
    return jnp.minimum(jnp.maximum(drawn, -limit), limit).astype(kind)


def setup_inputs(seed: int = 0, part: int = 0) -> dict:
    arg_keys = jax.random.split(jax.random.key(seed), 6)
    own_keys = jax.random.split(jax.random.fold_in(arg_keys[5], part), 6)
    return {
        "displacement": noise(own_keys[0], (3, NX, NY, NZ), 0.05, 0.75, ((1, 8),), jnp.float32),
        "velocity": draw_velocity(jax.random.fold_in(jax.random.fold_in(arg_keys[5], part), 71), part),
        "bond_mask": draw_bond_mask(jax.random.fold_in(jax.random.fold_in(arg_keys[5], part), 71), part),
        "moduli": jnp.clip(jnp.exp(jax.random.uniform(arg_keys[3], (MATS, 2), jnp.float32, math.log(16.0), math.log(64.0))), 16.0, 64.0),
        "material": jax.random.randint(own_keys[4], (1,), 0, MATS).astype(jnp.int32),
    }


time_step = 0.125

def half_list():
    found = []
    for a in range(-3, 4):
        for b in range(-3, 4):
            for c in range(-3, 4):
                if a * a + b * b + c * c <= 9 and (a, b, c) > (0, 0, 0):
                    found.append((a, b, c))
    return found

def offset_list():
    upward = half_list()
    return upward + [(-a, -b, -c) for a, b, c in upward]

def inside(coords, count):
    return jnp.logical_and(coords >= 0, coords < count).astype(jnp.float32)

def weighted_volume(coord_x, coord_y, coord_z, cells_x, cells_y, cells_z):
    summed = jnp.zeros((coord_x.shape[0], coord_y.shape[0], coord_z.shape[0]), jnp.float32)
    for a, b, c in offset_list():
        radius_sq = a * a + b * b + c * c
        factor = math.exp(-radius_sq / 9.0) * radius_sq
        summed = summed + factor * (inside(coord_x + a, cells_x)[:, None, None] * inside(coord_y + b, cells_y)[None, :, None] * inside(coord_z + c, cells_z)[None, None, :])
    home = inside(coord_x, cells_x)[:, None, None] * inside(coord_y, cells_y)[None, :, None] * inside(coord_z, cells_z)[None, None, :]
    return jnp.where(home > 0.5, summed, 1.0)

def bond_bit(bond_mask, k):
    return jnp.bitwise_and(jnp.right_shift(bond_mask[k // 16], k % 16), 1).astype(jnp.float32)

def bond_shape(here, across, a, b, c):
    bond_x = a + across[0] - here[0]
    bond_y = b + across[1] - here[1]
    bond_z = c + across[2] - here[2]
    length = jnp.sqrt(bond_x * bond_x + bond_y * bond_y + bond_z * bond_z)
    return (bond_x, bond_y, bond_z, length)

def window(array, a, b, c, own_x, cells_y, cells_z):
    return array[..., 3 + a:3 + a + own_x, 3 + b:3 + b + cells_y, 3 + c:3 + c + cells_z]

def reach_factor(inside_x, inside_y, inside_z, a, b, c, own_x, cells_y, cells_z):
    return inside_x[3 + a:3 + a + own_x][:, None, None] * inside_y[3 + b:3 + b + cells_y][None, :, None] * inside_z[3 + c:3 + c + cells_z][None, None, :]

def bond_pulls(extension, radius, weight, dilation_here, volume_here, dilation_across, volume_across, bulk_modulus, shear_modulus):
    deviation_here = extension - dilation_here * radius / 3.0
    deviation_across = extension - dilation_across * radius / 3.0
    pull_here = 3.0 * bulk_modulus * weight * radius * dilation_here / volume_here + 15.0 * shear_modulus * weight * deviation_here / volume_here
    pull_across = 3.0 * bulk_modulus * weight * radius * dilation_across / volume_across + 15.0 * shear_modulus * weight * deviation_across / volume_across
    return (deviation_here, deviation_across, pull_here + pull_across)

def dilatation(here, padded, bond_mask, inside_x, inside_y, inside_z, volume):
    own_x, cells_y, cells_z = here.shape[1:]
    summed = jnp.zeros((own_x, cells_y, cells_z), jnp.float32)
    for k, (a, b, c) in enumerate(offset_list()):
        radius = math.sqrt(a * a + b * b + c * c)
        factor = math.exp(-(a * a + b * b + c * c) / 9.0) * radius
        across = window(padded, a, b, c, own_x, cells_y, cells_z)
        intact = bond_bit(bond_mask, k) * reach_factor(inside_x, inside_y, inside_z, a, b, c, own_x, cells_y, cells_z)
        bond_x, bond_y, bond_z, length = bond_shape(here, across, a, b, c)
        summed = summed + intact * factor * (length - radius)
    return 3.0 * summed / volume

def stencil_forces(here, padded, bond_mask, inside_x, inside_y, inside_z, volume, volume_pad, dilation, dilation_pad, bulk_modulus, shear_modulus):
    own_x, cells_y, cells_z = here.shape[1:]
    force_x = jnp.zeros((own_x, cells_y, cells_z), jnp.float32)
    force_y = jnp.zeros((own_x, cells_y, cells_z), jnp.float32)
    force_z = jnp.zeros((own_x, cells_y, cells_z), jnp.float32)
    strain = jnp.zeros((own_x, cells_y, cells_z), jnp.float32)
    for k, (a, b, c) in enumerate(offset_list()):
        radius = math.sqrt(a * a + b * b + c * c)
        weight = math.exp(-(a * a + b * b + c * c) / 9.0)
        across = window(padded, a, b, c, own_x, cells_y, cells_z)
        intact = bond_bit(bond_mask, k) * reach_factor(inside_x, inside_y, inside_z, a, b, c, own_x, cells_y, cells_z)
        bond_x, bond_y, bond_z, length = bond_shape(here, across, a, b, c)
        dilation_across = window(dilation_pad, a, b, c, own_x, cells_y, cells_z)
        volume_across = window(volume_pad, a, b, c, own_x, cells_y, cells_z)
        deviation_here, deviation_across, pulls = bond_pulls(length - radius, radius, weight, dilation, volume, dilation_across, volume_across, bulk_modulus, shear_modulus)
        scaled = intact * pulls / length
        force_x = force_x + scaled * bond_x
        force_y = force_y + scaled * bond_y
        force_z = force_z + scaled * bond_z
        strain = strain + intact * weight * deviation_here * deviation_here
    density = 0.5 * bulk_modulus * dilation * dilation + 7.5 * shear_modulus * strain / volume
    return (jnp.stack([force_x, force_y, force_z]), density)

def material_moduli(moduli, material):
    chosen = (jnp.arange(moduli.shape[0], dtype=jnp.int32) == material[0]).astype(jnp.float32)
    return (jnp.sum(chosen * moduli[:, 0]), jnp.sum(chosen * moduli[:, 1]))

def reference(displacement, velocity, bond_mask, moduli, material):
    cells_x, cells_y, cells_z = displacement.shape[1:]
    bulk_modulus, shear_modulus = material_moduli(moduli, material)
    coord_x = jnp.arange(-3, cells_x + 3, dtype=jnp.int32)
    coord_y = jnp.arange(-3, cells_y + 3, dtype=jnp.int32)
    coord_z = jnp.arange(-3, cells_z + 3, dtype=jnp.int32)
    inside_x = inside(coord_x, cells_x)
    inside_y = inside(coord_y, cells_y)
    inside_z = inside(coord_z, cells_z)
    volume_pad = weighted_volume(coord_x, coord_y, coord_z, cells_x, cells_y, cells_z)
    volume = volume_pad[3:3 + cells_x, 3:3 + cells_y, 3:3 + cells_z]
    padded = jnp.pad(displacement, ((0, 0), (3, 3), (3, 3), (3, 3)))
    dilation = dilatation(displacement, padded, bond_mask, inside_x, inside_y, inside_z, volume)
    dilation_pad = jnp.pad(dilation, 3)
    force, density = stencil_forces(displacement, padded, bond_mask, inside_x, inside_y, inside_z, volume, volume_pad, dilation, dilation_pad, bulk_modulus, shear_modulus)
    new_velocity = velocity + time_step * force
    new_displacement = displacement + time_step * new_velocity
    summed = jnp.sum(0.5 * lax.optimization_barrier(jnp.sum(new_velocity * new_velocity, axis=0)) + density)
    energy = (summed / (cells_x * cells_y * cells_z)).reshape(1)
    return (new_displacement, new_velocity, energy)
```

```python
import functools
import math

import jax
import jax.numpy as jnp
import numpy as np
from jax import lax
from jax.experimental import pallas as pl
from jax.experimental.pallas import tpu as pltpu
from jax.sharding import PartitionSpec as P

DT = 0.125
MESH = pl.DeviceIdType.MESH
F32 = jnp.float32


def offset_list():
    up = []
    for a in range(-3, 4):
        for b in range(-3, 4):
            for c in range(-3, 4):
                if a * a + b * b + c * c <= 9 and (a, b, c) > (0, 0, 0):
                    up.append((a, b, c))
    return up + [(-a, -b, -c) for a, b, c in up]


OFFSETS = offset_list()
NUMBER = {o: k for k, o in enumerate(OFFSETS)}
SLOT = {o: k for k, o in enumerate(sorted(OFFSETS))}


def classes(a):
    found = {}
    for o in sorted(OFFSETS):
        if o[0] == a:
            found.setdefault(a * a + o[1] * o[1] + o[2] * o[2], []).append(o)
    return sorted(found.items())


def signed(bits):
    bits &= 0xFFFFFFFF
    return bits - (1 << 32) if bits >> 31 else bits


def tables(nx, ny, nz, words):
    in_x = np.zeros((nx, words), np.int64)
    in_y = np.zeros((ny, words), np.int64)
    in_z = np.zeros((nz, words), np.int64)
    plane = np.zeros((4, ny, nz), np.float64)
    y, z = np.arange(ny), np.arange(nz)
    for k, (a, b, c) in enumerate(OFFSETS):
        w, bit = k // 16, 1 << (k % 16)
        for x in range(nx):
            in_x[x, w] |= bit * (0 <= x + a < nx)
        ok_y = (0 <= y + b) & (y + b < ny)
        ok_z = (0 <= z + c) & (z + c < nz)
        in_y[:, w] |= bit * ok_y
        in_z[:, w] |= bit * ok_z
        if a >= 0:
            r2 = a * a + b * b + c * c
            plane[a] += math.exp(-r2 / 9.0) * r2 * (ok_y[:, None] & ok_z[None, :])
    in_yz = in_y.T[:, :, None] & in_z.T[:, None, :]
    return in_x.astype(np.int32), in_yz.astype(np.int32), plane.astype(np.float32)


def kernel(
    sx, nx,
    u_hbm, v_hbm, w_hbm, yz_hbm, plane_hbm, moduli, material, in_x,
    nu_hbm, nv_hbm, en_ref,
    U, S, HY, W, YZ, Q, AL, SA, SB, V, ACC, HM, E1, FA, VEL, OV, OU, EB, EP,
    local, out_sem, us, ur, fs, fr, ts, tr, gs, gr, es, er, ps, pr,
):
    ens = lax.axis_index("ens")
    slab = lax.axis_index("slab")
    nxs = sx // 2
    px = slab // 2
    par = slab % 2
    step = 1 - 2 * par
    partner = (ens, slab + step)
    ahead = (ens, slab + 2 * step)
    has_ahead = jnp.logical_and(px + step >= 0, px + step < nxs)
    has_behind = jnp.logical_and(px - step >= 0, px - step < nxs)
    own_x = U.shape[0] // 3
    ny, nz = U.shape[2:]

    def at_x(d):
        return (ens, 2 * ((px + d) % nxs) + par)

    barrier = pltpu.get_barrier_semaphore()
    pl.semaphore_signal(barrier, inc=1, device_id=partner, device_id_type=MESH)
    for d in range(1, nxs):
        pl.semaphore_signal(barrier, inc=1, device_id=at_x(d), device_id_type=MESH)

    def layer(i):
        return i + par * (own_x - 1 - 2 * i)

    loads = []

    def load(src, dst):
        c = pltpu.make_async_copy(src, dst, local.at[len(loads)])
        c.start()
        loads.append(c)
        return c

    u_loads = [load(u_hbm.at[:, layer(i)], U.at[own_x + i]) for i in range(own_x)]
    w_loads = [load(w_hbm.at[:, layer(i)], W.at[i]) for i in range(own_x)]
    w_loads.append(load(yz_hbm, YZ))
    q_load = load(plane_hbm, Q)
    v_loads = [load(v_hbm.at[:, layer(i)], VEL.at[i]) for i in range(own_x)]

    def remote(src, dst, send, recv, dev):
        return pltpu.make_async_remote_copy(
            src_ref=src, dst_ref=dst, send_sem=send, recv_sem=recv, device_id=dev, device_id_type=MESH
        )

    def to_partner(ref, send, recv, i):
        return remote(ref.at[own_x + i], ref.at[3 * own_x - 1 - i], send.at[i], recv.at[i], partner)

    def to_ahead(ref, send, recv, i):
        return remote(ref.at[3 * own_x - 1 - i], ref.at[own_x - 1 - i], send.at[i], recv.at[i], ahead)

    for c in u_loads:
        c.wait()
    pl.semaphore_wait(barrier, nxs)
    for i in range(own_x):
        to_partner(U, us, ur, i).start()

    sign = step.astype(F32)
    bulk = moduli[material[0], 0]
    shear = moduli[material[0], 1]
    zero = jnp.zeros((8, nz), F32)

    def clear(L, _):
        for c in range(7):
            for comp in range(3):
                S[c, L, comp, 0:8] = zero
                S[c, L, comp, 8 + ny : 16 + ny] = zero
            for ref in (SA, SB):
                ref[c, L, 0:8] = zero
                ref[c, L, 8 + ny : 16 + ny] = zero
        return 0

    lax.fori_loop(0, 3 * own_x, clear, 0)

    @pl.when(jnp.logical_not(has_behind))
    def _():
        for L in range(own_x):
            for comp in range(3):
                U[L, comp] = jnp.zeros((ny, nz), F32)
            AL[L] = jnp.zeros((ny, nz), F32)

    def rolled(x, c):
        return x if c == 0 else pltpu.roll(x, (-c) % nz, 1)

    def shift_u(L, reach):
        ux = U[L, 0] * sign
        uy = U[L, 1]
        uz = U[L, 2]
        for c in range(-reach, reach + 1):
            S[c + 3, L, 0, 8 : 8 + ny] = rolled(ux, c)
            S[c + 3, L, 1, 8 : 8 + ny] = rolled(uy, c)
            S[c + 3, L, 2, 8 : 8 + ny] = rolled(uz, c) + float(c)

    def shift_to(ref, L, x, reach):
        for c in range(-reach, reach + 1):
            ref[c + 3, L, 8 : 8 + ny] = rolled(x, c)

    def prepare(i, _):
        shift_u(own_x + i, 3)
        uy = U[own_x + i, 1]
        for b in range(-3, 4):
            HY[b + 3, i] = uy - float(b)
        for n in range(3):
            ACC[n, i] = jnp.zeros((ny, nz), F32)
            FA[n, i] = jnp.zeros((ny, nz), F32)
        return 0

    lax.fori_loop(0, own_x, prepare, 0)
    for c in w_loads:
        c.wait()
    base = own_x * slab

    def clean(i, _):
        x = base + layer(i)
        for n in range(W.shape[1]):
            W[i, n] = W[i, n] & YZ[n] & in_x[x * W.shape[1] + n]
        return 0

    lax.fori_loop(0, own_x, clean, 0)

    def bond(a, b, c, i, L, hx, hz):
        rows = slice(8 + b, 8 + b + ny)
        bx = S[c + 3, L, 0, rows] - hx
        by = S[c + 3, L, 1, rows] - HY[b + 3, i]
        bz = S[c + 3, L, 2, rows] - hz
        return bx, by, bz

    def first(a, i):
        L = own_x + i + a
        hx = U[own_x + i, 0] * sign - float(a)
        hz = U[own_x + i, 2]
        total = [jnp.zeros((ny, nz), F32)] * 3
        for r2, offs in classes(a):
            r, wt = math.sqrt(r2), math.exp(-r2 / 9.0)
            s1 = s2 = s0 = None
            for _, b, c in offs:
                bx, by, bz = bond(a, b, c, i, L, hx, hz)
                sq = bx * bx + by * by + bz * bz
                inv = lax.rsqrt(sq)
                st = sq * inv - r
                kp, km = NUMBER[(a, b, c)], NUMBER[(-a, b, c)]
                word = kp // 16 + par * (km // 16 - kp // 16)
                bit = (1 << (kp % 16)) + par * ((1 << (km % 16)) - (1 << (kp % 16)))
                live = (W[i, word] & bit) != 0
                ms = jnp.where(live, st, 0.0)
                hm = jnp.where(live, inv, 0.0)
                one = jnp.where(live, 1.0, 0.0)
                HM[SLOT[(a, b, c)], i] = hm * r
                E1[SLOT[(a, b, c)], i] = ms * hm
                s1 = ms if s1 is None else s1 + ms
                s2 = ms * ms if s2 is None else s2 + ms * ms
                s0 = one if s0 is None else s0 + one
            total = [total[0] + (wt * r) * s1, total[1] + wt * s2, total[2] + (wt * r2) * s0]
        for n in range(3):
            ACC[n, i] += total[n]

    def second(a, i):
        L = own_x + i + a
        hx = U[own_x + i, 0] * sign - float(a)
        hz = U[own_x + i, 2]
        ah = AL[own_x + i]
        bh = SB[3, own_x + i, 8 : 8 + ny]
        total = [jnp.zeros((ny, nz), F32)] * 3
        for r2, offs in classes(a):
            wt = math.exp(-r2 / 9.0)
            f = [None] * 3
            for _, b, c in offs:
                rows = slice(8 + b, 8 + b + ny)
                k = SLOT[(a, b, c)]
                t = (bh + SB[c + 3, L, rows]) * E1[k, i] + (ah + SA[c + 3, L, rows]) * HM[k, i]
                y = bond(a, b, c, i, L, hx, hz)
                f = [t * y[n] if f[n] is None else f[n] + t * y[n] for n in range(3)]
            total = [total[n] + wt * f[n] for n in range(3)]
        for n in range(3):
            FA[n, i] += total[n]

    def inner(block):
        def at(a, lo, hi):
            def one(i, _):
                block(a, i)
                return 0

            lax.fori_loop(lo, hi, one, 0)

        for a in range(-2, 3):
            at(a, max(0, -a), own_x - max(0, a))

    def outer(block, L):
        for i in range(own_x):
            a = L - own_x - i
            if -3 <= a <= 3:
                block(a, i)

    inner(first)

    q_load.wait()

    def volumes(L, _):
        x = base + layer(L - own_x)
        sums = jnp.zeros((ny, nz), F32)
        for a in range(4):
            up = jnp.logical_and(x + a >= 0, x + a < nx).astype(F32)
            down = jnp.logical_and(x - a >= 0, x - a < nx).astype(F32)
            sums = sums + (up if a == 0 else up + down) * Q[a]
        home = jnp.logical_and(x >= 0, x < nx)
        vol = jnp.where(home, sums, 1.0)
        V[L] = vol
        shift_to(SB, L, 15.0 * shear / vol, 3)
        return 0

    lax.fori_loop(0, 3 * own_x, volumes, 0)

    for i in range(own_x):
        L = 3 * own_x - 1 - i
        to_partner(U, us, ur, i).wait_recv()

        @pl.when(has_ahead)
        def _():
            to_ahead(U, fs, fr, i).start()

        shift_u(L, 2)
        outer(first, L)
    for i in range(own_x):
        L = own_x - 1 - i

        @pl.when(has_behind)
        def _():
            to_ahead(U, fs, fr, i).wait_recv()

        shift_u(L, 2)
        outer(first, L)

    factor = 3.0 * bulk - 5.0 * shear

    def dilate(i, _):
        vol = V[own_x + i]
        AL[own_x + i] = factor * (3.0 * ACC[0, i] / vol) / vol
        return 0

    lax.fori_loop(0, own_x, dilate, 0)

    def shift_a(i, _):
        shift_to(SA, own_x + i, AL[own_x + i], 3)
        return 0

    lax.fori_loop(0, own_x, shift_a, 0)
    for i in range(own_x):
        to_partner(AL, ts, tr, i).start()

    inner(second)

    for i in range(own_x):
        L = 3 * own_x - 1 - i
        to_partner(AL, ts, tr, i).wait_recv()

        @pl.when(has_ahead)
        def _():
            to_ahead(AL, gs, gr, i).start()

        shift_to(SA, L, AL[L], 2)
        outer(second, L)
    for i in range(own_x):
        L = own_x - 1 - i

        @pl.when(has_behind)
        def _():
            to_ahead(AL, gs, gr, i).wait_recv()

        shift_to(SA, L, AL[L], 2)
        outer(second, L)

    for c in v_loads:
        c.wait()
    heat = jnp.zeros((ny, nz), F32)
    for i in range(own_x):
        kinetic = None
        for n in range(3):
            force = FA[n, i] * sign if n == 0 else FA[n, i]
            nv = VEL[i, n] + DT * force
            OV[i, n] = nv
            OU[i, n] = U[own_x + i, n] + DT * nv
            kinetic = nv * nv if kinetic is None else kinetic + nv * nv
        vol = V[own_x + i]
        th = 3.0 * ACC[0, i] / vol
        th2 = th * th
        strain = ACC[1, i] - (2.0 / 9.0) * th2 * vol + th2 * ACC[2, i] * (1.0 / 9.0)
        heat = heat + 0.5 * kinetic + 0.5 * bulk * th2 + 7.5 * shear * strain / vol
    EB[px] = jnp.sum(heat, axis=0, keepdims=True)

    outs = []
    for i in range(own_x):
        for src, dst in ((OV, nv_hbm), (OU, nu_hbm)):
            c = pltpu.make_async_copy(src.at[i], dst.at[:, layer(i)], out_sem.at[len(outs)])
            c.start()
            outs.append(c)

    rows = [remote(EB.at[px], EB.at[px], es.at[d], er.at[px], at_x(d)) for d in range(1, nxs)]
    for c in rows:
        c.start()
    for d in range(1, nxs):
        q = (px + d) % nxs
        remote(EB.at[q], EB.at[q], es.at[d], er.at[q], at_x(d)).wait_recv()
    group = EB[0]
    for n in range(1, nxs):
        group = group + EB[n]
    EP[0] = group
    last = remote(EP.at[0], EP.at[1], ps, pr, partner)
    last.start()
    for c in outs:
        c.wait()
    for i in range(own_x):
        to_partner(U, us, ur, i).wait_send()
        to_partner(AL, ts, tr, i).wait_send()

        @pl.when(has_ahead)
        def _():
            to_ahead(U, fs, fr, i).wait_send()
            to_ahead(AL, gs, gr, i).wait_send()

    for c in rows:
        c.wait_send()
    last.wait_recv()
    both = EP[0] + EP[1]
    en_ref[...] = jnp.broadcast_to(jnp.sum(both, axis=1, keepdims=True), en_ref.shape) * (1.0 / (nx * ny * nz))
    last.wait_send()


def solution(mesh):
    slabs = mesh.shape["slab"]

    def body(displacement, velocity, bond_mask, moduli, material):
        own_x, ny, nz = displacement.shape[1:]
        words = bond_mask.shape[0]
        nx = own_x * slabs
        in_x, in_yz, plane = tables(nx, ny, nz, words)
        grid = (ny, nz)
        tall = (ny + 16, nz)
        nb = len(OFFSETS)
        vm = pltpu.VMEM
        dma = pltpu.SemaphoreType.DMA
        hbm = pl.BlockSpec(memory_space=pl.ANY)
        smem = pl.BlockSpec(memory_space=pltpu.SMEM)
        full = jax.ShapeDtypeStruct(displacement.shape, F32)
        nu, nv, en = pl.pallas_call(
            functools.partial(kernel, slabs, nx),
            out_shape=(full, full, jax.ShapeDtypeStruct((1, nz), F32)),
            in_specs=[hbm] * 5 + [smem] * 3,
            out_specs=(hbm, hbm, pl.BlockSpec(memory_space=pltpu.VMEM)),
            scratch_shapes=[
                vm((3 * own_x, 3) + grid, F32),
                vm((7, 3 * own_x, 3) + tall, F32),
                vm((7, own_x) + grid, F32),
                vm((own_x, words) + grid, jnp.int32),
                vm((words,) + grid, jnp.int32),
                vm((4,) + grid, F32),
                vm((3 * own_x,) + grid, F32),
                vm((7, 3 * own_x) + tall, F32),
                vm((7, 3 * own_x) + tall, F32),
                vm((3 * own_x,) + grid, F32),
                vm((3, own_x) + grid, F32),
                vm((nb, own_x) + grid, F32),
                vm((nb, own_x) + grid, F32),
                vm((3, own_x) + grid, F32),
                vm((own_x, 3) + grid, F32),
                vm((own_x, 3) + grid, F32),
                vm((own_x, 3) + grid, F32),
                vm((slabs // 2, 1, nz), F32),
                vm((2, 1, nz), F32),
                dma((3 * own_x + 2,)),
                dma((2 * own_x,)),
                dma((own_x,)), dma((own_x,)), dma((own_x,)), dma((own_x,)),
                dma((own_x,)), dma((own_x,)), dma((own_x,)), dma((own_x,)),
                dma((slabs // 2,)), dma((slabs // 2,)),
                dma, dma,
            ],
            compiler_params=pltpu.CompilerParams(collective_id=0, has_side_effects=True),
        )(
            displacement, velocity, bond_mask, jnp.asarray(in_yz), jnp.asarray(plane),
            moduli, material, jnp.asarray(in_x.reshape(-1)),
        )
        return nu, nv, en[0, :1]

    in_specs = (
        P("ens", "slab", None, None),
        P("ens", "slab", None, None),
        P("ens", "slab", None, None),
        P(),
        P("ens"),
    )
    out_specs = (P("ens", "slab", None, None), P("ens", "slab", None, None), P("ens"))
    return jax.shard_map(body, mesh=mesh, in_specs=in_specs, out_specs=out_specs, check_vma=False)
```

```python
import functools
import math

import jax
import jax.numpy as jnp
import numpy as np
from jax import lax
from jax.experimental import pallas as pl
from jax.experimental.pallas import tpu as pltpu
from jax.sharding import PartitionSpec as P

DT = 0.125
MESH = pl.DeviceIdType.MESH
F32 = jnp.float32


def offset_list():
    up = []
    for a in range(-3, 4):
        for b in range(-3, 4):
            for c in range(-3, 4):
                if a * a + b * b + c * c <= 9 and (a, b, c) > (0, 0, 0):
                    up.append((a, b, c))
    return up + [(-a, -b, -c) for a, b, c in up]


OFFSETS = offset_list()
NUMBER = {o: k for k, o in enumerate(OFFSETS)}
SLOT = {o: k for k, o in enumerate(sorted(OFFSETS))}


def classes(a):
    found = {}
    for o in sorted(OFFSETS):
        if o[0] == a:
            found.setdefault(a * a + o[1] * o[1] + o[2] * o[2], []).append(o)
    return sorted(found.items())


def layer_bits(a, word):
    return sum(1 << (k % 16) for k, o in enumerate(OFFSETS) if o[0] == a and k // 16 == word)


def tables(ny, nz, words):
    in_y = np.zeros((ny, words), np.int64)
    in_z = np.zeros((nz, words), np.int64)
    plane = np.zeros((4, ny, nz), np.float64)
    y, z = np.arange(ny), np.arange(nz)
    for k, (a, b, c) in enumerate(OFFSETS):
        w, bit = k // 16, 1 << (k % 16)
        ok_y = (0 <= y + b) & (y + b < ny)
        ok_z = (0 <= z + c) & (z + c < nz)
        in_y[:, w] |= bit * ok_y
        in_z[:, w] |= bit * ok_z
        if a >= 0:
            r2 = a * a + b * b + c * c
            plane[a] += math.exp(-r2 / 9.0) * r2 * (ok_y[:, None] & ok_z[None, :])
    in_yz = in_y.T[:, :, None] & in_z.T[:, None, :]
    return in_yz.astype(np.int32), plane.astype(np.float32)


def kernel(
    sx, nx,
    u_hbm, v_hbm, w_hbm, yz_hbm, plane_hbm, moduli_hbm, material_hbm,
    force_hbm, en_ref,
    U, S, HY, W, WS, YZ, Q, SI, CX, RX, AL, SA, SB, V, ACC, HM, E1, FA, VEL, FO, EB, moduli, material,
    local, out_sem, us, ur, fs, fr, ts, tr, gs, gr, xs, xr, es, er,
):
    ens = lax.axis_index("ens")
    slab = lax.axis_index("slab")
    nxs = sx // 2
    px = slab // 2
    par = slab % 2
    step = 1 - 2 * par
    partner = (ens, slab + step)
    ahead = (ens, slab + 2 * step)
    behind = (ens, slab - 2 * step)
    has_ahead = jnp.logical_and(px + step >= 0, px + step < nxs)
    has_behind = jnp.logical_and(px - step >= 0, px - step < nxs)
    own_x = U.shape[0] // 3
    ny, nz = U.shape[2:]

    def slab_at(d, other):
        return 2 * ((px + d) % nxs) + (1 - par if other else par)

    def at_x(d):
        return (ens, slab_at(d, False))

    barrier = pltpu.get_barrier_semaphore()
    pl.semaphore_signal(barrier, inc=1, device_id=partner, device_id_type=MESH)
    for d in range(1, nxs):
        pl.semaphore_signal(barrier, inc=1, device_id=at_x(d), device_id_type=MESH)

    def layer(i):
        return i + par * (own_x - 1 - 2 * i)

    loads = []

    def load(src, dst):
        c = pltpu.make_async_copy(src, dst, local.at[len(loads)])
        c.start()
        loads.append(c)
        return c

    u_loads = [load(u_hbm.at[:, layer(i)], U.at[own_x + i]) for i in range(own_x)]
    w_loads = [load(w_hbm.at[:, layer(i)], W.at[i]) for i in range(own_x)]
    w_loads.append(load(yz_hbm, YZ))
    q_loads = [load(plane_hbm, Q), load(moduli_hbm, moduli), load(material_hbm, material)]
    v_loads = [load(v_hbm.at[:, layer(i)], VEL.at[i]) for i in range(own_x)]

    def remote(src, dst, send, recv, dev):
        return pltpu.make_async_remote_copy(
            src_ref=src, dst_ref=dst, send_sem=send, recv_sem=recv, device_id=dev, device_id_type=MESH
        )

    def to_partner(ref, send, recv, i):
        return remote(ref.at[own_x + i], ref.at[3 * own_x - 1 - i], send.at[i], recv.at[i], partner)

    def to_ahead(ref, send, recv, i):
        return remote(ref.at[3 * own_x - 1 - i], ref.at[own_x - 1 - i], send.at[i], recv.at[i], ahead)

    for L in range(own_x):

        @pl.when(jnp.logical_not(has_behind))
        def _():
            RX[L] = jnp.zeros((ny, nz), F32)

        @pl.when(jnp.logical_not(has_ahead))
        def _():
            RX[2 * own_x + L] = jnp.zeros((ny, nz), F32)

    for c in u_loads:
        c.wait()
    pl.semaphore_wait(barrier, nxs)
    for i in range(own_x):
        to_partner(U, us, ur, i).start()

    sign = step.astype(F32)
    zero = jnp.zeros((8, nz), F32)

    def clear(L, _):
        for c in range(7):
            for comp in range(3):
                S[c, L, comp, 0:8] = zero
                S[c, L, comp, 8 + ny : 16 + ny] = zero
            for ref in (SA, SB):
                ref[c, L, 0:8] = zero
                ref[c, L, 8 + ny : 16 + ny] = zero
        return 0

    lax.fori_loop(0, 3 * own_x, clear, 0)

    @pl.when(jnp.logical_not(has_behind))
    def _():
        for L in range(own_x):
            for comp in range(3):
                U[L, comp] = jnp.zeros((ny, nz), F32)
            SI[L] = jnp.zeros((ny, nz), F32)

    def rolled(x, c):
        return x if c == 0 else pltpu.roll(x, (-c) % nz, 1)

    def shift_u(L, reach):
        ux = U[L, 0] * sign
        uy = U[L, 1]
        uz = U[L, 2]
        for c in range(-reach, reach + 1):
            S[c + 3, L, 0, 8 : 8 + ny] = rolled(ux, c)
            S[c + 3, L, 1, 8 : 8 + ny] = rolled(uy, c)
            S[c + 3, L, 2, 8 : 8 + ny] = rolled(uz, c) + float(c)

    def shift_to(ref, L, x, reach):
        for c in range(-reach, reach + 1):
            ref[c + 3, L, 8 : 8 + ny] = rolled(x, c)

    def prepare(i, _):
        shift_u(own_x + i, 3)
        uy = U[own_x + i, 1]
        for b in range(-3, 4):
            HY[b + 3, i] = uy - float(b)
        for n in range(3):
            ACC[n, i] = jnp.zeros((ny, nz), F32)
            FA[n, i] = jnp.zeros((ny, nz), F32)
        return 0

    lax.fori_loop(0, own_x, prepare, 0)
    for c in w_loads:
        c.wait()
    base = own_x * slab

    def clean(i, _):
        x = base + layer(i)
        gone = {a: jnp.logical_or(x + a < 0, x + a >= nx).astype(jnp.int32) for a in range(-3, 4) if a}
        for n in range(W.shape[1]):
            keep = 0xFFFF
            for a, out in gone.items():
                if layer_bits(a, n):
                    keep = keep - out * layer_bits(a, n)
            word = W[i, n] & YZ[n] & keep
            W[i, n] = word
            for c in range(-2, 3):
                WS[c + 2, i, n, 0:8] = jnp.zeros((8, nz), jnp.int32)
                WS[c + 2, i, n, 8 + ny : 16 + ny] = jnp.zeros((8, nz), jnp.int32)
                WS[c + 2, i, n, 8 : 8 + ny] = rolled(word, c)
        return 0

    lax.fori_loop(0, own_x, clean, 0)

    def bond(a, b, c, i, L, hx, hz):
        rows = slice(8 + b, 8 + b + ny)
        bx = S[c + 3, L, 0, rows] - hx
        by = S[c + 3, L, 1, rows] - HY[b + 3, i]
        bz = S[c + 3, L, 2, rows] - hz
        return bx, by, bz

    def where_bit(a, b, c):
        kp, km = NUMBER[(a, b, c)], NUMBER[(-a, b, c)]
        word = kp // 16 + par * (km // 16 - kp // 16)
        bit = (1 << (kp % 16)) + par * ((1 << (km % 16)) - (1 << (kp % 16)))
        return word, bit

    def across(a, i):
        L = own_x + i + a
        hx = U[L, 0] * sign + float(a)
        hy = U[L, 1]
        hz = U[L, 2]
        total = None
        for r2, offs in classes(a):
            r, wt = math.sqrt(r2), math.exp(-r2 / 9.0)
            s1 = None
            for _, b, c in offs:
                rows = slice(8 - b, 8 - b + ny)
                bx = S[3 - c, own_x + i, 0, rows] - hx
                by = S[3 - c, own_x + i, 1, rows] - (hy + float(b))
                bz = S[3 - c, own_x + i, 2, rows] - hz
                sq = bx * bx + by * by + bz * bz
                st = sq * lax.rsqrt(sq) - r
                word, bit = where_bit(a, b, c)
                live = (WS[2 - c, i, word, rows] & bit) != 0
                ms = jnp.where(live, st, 0.0)
                s1 = ms if s1 is None else s1 + ms
            total = (wt * r) * s1 if total is None else total + (wt * r) * s1
        return total

    def first(a, i):
        L = own_x + i + a
        hx = U[own_x + i, 0] * sign - float(a)
        hz = U[own_x + i, 2]
        total = [jnp.zeros((ny, nz), F32)] * 3
        for r2, offs in classes(a):
            r, wt = math.sqrt(r2), math.exp(-r2 / 9.0)
            s1 = s2 = s0 = None
            for _, b, c in offs:
                bx, by, bz = bond(a, b, c, i, L, hx, hz)
                sq = bx * bx + by * by + bz * bz
                inv = lax.rsqrt(sq)
                st = sq * inv - r
                word, bit = where_bit(a, b, c)
                live = (W[i, word] & bit) != 0
                ms = jnp.where(live, st, 0.0)
                hm = jnp.where(live, inv, 0.0)
                one = jnp.where(live, 1.0, 0.0)
                HM[SLOT[(a, b, c)], i] = hm * r
                E1[SLOT[(a, b, c)], i] = ms * hm
                s1 = ms if s1 is None else s1 + ms
                s2 = ms * ms if s2 is None else s2 + ms * ms
                s0 = one if s0 is None else s0 + one
            total = [total[0] + (wt * r) * s1, total[1] + wt * s2, total[2] + (wt * r2) * s0]
        for n in range(3):
            ACC[n, i] += total[n]

    def second(a, i):
        L = own_x + i + a
        hx = U[own_x + i, 0] * sign - float(a)
        hz = U[own_x + i, 2]
        ah = AL[own_x + i]
        bh = SB[3, own_x + i, 8 : 8 + ny]
        total = [jnp.zeros((ny, nz), F32)] * 3
        for r2, offs in classes(a):
            wt = math.exp(-r2 / 9.0)
            f = [None] * 3
            for _, b, c in offs:
                rows = slice(8 + b, 8 + b + ny)
                k = SLOT[(a, b, c)]
                t = (bh + SB[c + 3, L, rows]) * E1[k, i] + (ah + SA[c + 3, L, rows]) * HM[k, i]
                y = bond(a, b, c, i, L, hx, hz)
                f = [t * y[n] if f[n] is None else f[n] + t * y[n] for n in range(3)]
            total = [total[n] + wt * f[n] for n in range(3)]
        for n in range(3):
            FA[n, i] += total[n]

    def inner(block):
        def at(a, lo, hi):
            def one(i, _):
                block(a, i)
                return 0

            lax.fori_loop(lo, hi, one, 0)

        for a in range(-2, 3):
            at(a, max(0, -a), own_x - max(0, a))

    def outer(block, L):
        for i in range(own_x):
            a = L - own_x - i
            if -3 <= a <= 3:
                block(a, i)

    inner(first)
    for i in range(own_x):
        SI[own_x + i] = ACC[0, i]

    for c in q_loads:
        c.wait()
    bulk = moduli[0, material[0]]
    shear = moduli[1, material[0]]
    factor = 3.0 * bulk - 5.0 * shear

    def volumes(L, _):
        x = base + layer(L - own_x)
        sums = jnp.zeros((ny, nz), F32)
        for a in range(4):
            up = jnp.logical_and(x + a >= 0, x + a < nx).astype(F32)
            down = jnp.logical_and(x - a >= 0, x - a < nx).astype(F32)
            sums = sums + (up if a == 0 else up + down) * Q[a]
        home = jnp.logical_and(x >= 0, x < nx)
        vol = jnp.where(home, sums, 1.0)
        V[L] = vol
        shift_to(SB, L, 15.0 * shear / vol, 3)
        return 0

    lax.fori_loop(0, own_x, volumes, 0)
    for i in range(own_x):
        to_partner(SI, ts, tr, i).start()
    lax.fori_loop(own_x, 3 * own_x, volumes, 0)

    def arrived(L):
        shift_u(L, 2)
        outer(first, L)
        total = None
        for i in range(own_x):
            a = L - own_x - i
            if -3 <= a <= 3:
                part = across(a, i)
                total = part if total is None else total + part
        CX[L] = total

    for i in range(own_x):
        to_partner(U, us, ur, i).wait_recv()

        @pl.when(has_ahead)
        def _():
            to_ahead(U, fs, fr, i).start()

        arrived(3 * own_x - 1 - i)

    n = own_x
    part_up = remote(CX.at[pl.ds(2 * n, n)], RX.at[pl.ds(0, n)], xs.at[0], xr.at[0], ahead)
    part_down = remote(CX.at[pl.ds(0, n)], RX.at[pl.ds(2 * n, n)], xs.at[1], xr.at[1], behind)

    @pl.when(has_ahead)
    def _():
        part_up.start()

    for i in range(own_x):

        @pl.when(has_behind)
        def _():
            to_ahead(U, fs, fr, i).wait_recv()

        arrived(own_x - 1 - i)

    def dilate(i, _):
        vol = V[own_x + i]
        a = factor * (3.0 * ACC[0, i] / vol) / vol
        AL[own_x + i] = a
        shift_to(SA, own_x + i, a, 3)
        return 0

    lax.fori_loop(0, own_x, dilate, 0)

    @pl.when(has_behind)
    def _():
        part_down.start()

    for i in range(own_x):
        to_partner(SI, ts, tr, i).wait_recv()

        @pl.when(has_ahead)
        def _():
            to_ahead(SI, gs, gr, i).start()

    inner(second)

    def halo(L):
        vol = V[L]
        shift_to(SA, L, factor * (3.0 * (SI[L] + CX[L] + RX[L]) / vol) / vol, 2)
        outer(second, L)

    @pl.when(has_ahead)
    def _():
        part_down.wait_recv()

    for i in range(own_x):
        halo(3 * own_x - 1 - i)

    @pl.when(has_behind)
    def _():
        part_up.wait_recv()

    for i in range(own_x):

        @pl.when(has_behind)
        def _():
            to_ahead(SI, gs, gr, i).wait_recv()

        halo(own_x - 1 - i)

    for c in v_loads:
        c.wait()
    heat = jnp.zeros((ny, nz), F32)
    for i in range(own_x):
        kinetic = None
        for n in range(3):
            force = FA[n, i] * sign if n == 0 else FA[n, i]
            FO[i, n] = force
            nv = VEL[i, n] + DT * force
            kinetic = nv * nv if kinetic is None else kinetic + nv * nv
        vol = V[own_x + i]
        th = 3.0 * ACC[0, i] / vol
        th2 = th * th
        strain = ACC[1, i] - (2.0 / 9.0) * th2 * vol + th2 * ACC[2, i] * (1.0 / 9.0)
        heat = heat + 0.5 * kinetic + 0.5 * bulk * th2 + 7.5 * shear * strain / vol
    EB[slab] = jnp.sum(heat, axis=0, keepdims=True)

    outs = []
    for i in range(own_x):
        c = pltpu.make_async_copy(FO.at[i], force_hbm.at[:, layer(i)], out_sem.at[i])
        c.start()
        outs.append(c)

    peers = [(d, o) for o in (True, False) for d in range(nxs) if d or o]
    rows = []
    for n, (d, o) in enumerate(peers):
        c = remote(EB.at[slab], EB.at[slab], es.at[n], er.at[slab], (ens, slab_at(d, o)))
        c.start()
        rows.append(c)
    for c in outs:
        c.wait()
    for i in range(own_x):
        to_partner(U, us, ur, i).wait_send()
        to_partner(SI, ts, tr, i).wait_send()

        @pl.when(has_ahead)
        def _():
            to_ahead(U, fs, fr, i).wait_send()
            to_ahead(SI, gs, gr, i).wait_send()

    @pl.when(has_ahead)
    def _():
        part_up.wait_send()

    @pl.when(has_behind)
    def _():
        part_down.wait_send()

    for c in rows:
        c.wait_send()
    for n, (d, o) in enumerate(peers):
        q = slab_at(d, o)
        remote(EB.at[q], EB.at[q], es.at[n], er.at[q], (ens, q)).wait_recv()
    whole = EB[0]
    for n in range(1, sx):
        whole = whole + EB[n]
    en_ref[...] = jnp.broadcast_to(jnp.sum(whole, axis=1, keepdims=True), en_ref.shape) * (1.0 / (nx * ny * nz))


def solution(mesh):
    slabs = mesh.shape["slab"]

    def body(displacement, velocity, bond_mask, moduli, material):
        own_x, ny, nz = displacement.shape[1:]
        words = bond_mask.shape[0]
        nx = own_x * slabs
        in_yz, plane = tables(ny, nz, words)
        grid = (ny, nz)
        tall = (ny + 16, nz)
        nb = len(OFFSETS)
        vm = pltpu.VMEM
        dma = pltpu.SemaphoreType.DMA
        hbm = pl.BlockSpec(memory_space=pl.ANY)
        force, en = pl.pallas_call(
            functools.partial(kernel, slabs, nx),
            out_shape=(jax.ShapeDtypeStruct(displacement.shape, F32), jax.ShapeDtypeStruct((1, nz), F32)),
            in_specs=[hbm] * 7,
            out_specs=(hbm, pl.BlockSpec(memory_space=pltpu.VMEM)),
            scratch_shapes=[
                vm((3 * own_x, 3) + grid, F32),
                vm((7, 3 * own_x, 3) + tall, F32),
                vm((7, own_x) + grid, F32),
                vm((own_x, words) + grid, jnp.int32),
                vm((5, own_x, words) + tall, jnp.int32),
                vm((words,) + grid, jnp.int32),
                vm((4,) + grid, F32),
                vm((3 * own_x,) + grid, F32),
                vm((3 * own_x,) + grid, F32),
                vm((3 * own_x,) + grid, F32),
                vm((3 * own_x,) + grid, F32),
                vm((7, 3 * own_x) + tall, F32),
                vm((7, 3 * own_x) + tall, F32),
                vm((3 * own_x,) + grid, F32),
                vm((3, own_x) + grid, F32),
                vm((nb, own_x) + grid, F32),
                vm((nb, own_x) + grid, F32),
                vm((3, own_x) + grid, F32),
                vm((own_x, 3) + grid, F32),
                vm((own_x, 3) + grid, F32),
                vm((slabs, 1, nz), F32),
                pltpu.SMEM(moduli.shape[::-1], F32),
                pltpu.SMEM(material.shape, jnp.int32),
                dma((3 * own_x + 4,)),
                dma((own_x,)),
                dma((own_x,)), dma((own_x,)), dma((own_x,)), dma((own_x,)),
                dma((own_x,)), dma((own_x,)), dma((own_x,)), dma((own_x,)),
                dma((2,)), dma((2,)),
                dma((slabs,)), dma((slabs,)),
            ],
            compiler_params=pltpu.CompilerParams(collective_id=0, has_side_effects=True),
        )(
            displacement, velocity, bond_mask, jnp.asarray(in_yz), jnp.asarray(plane),
            moduli.T, material,
        )
        new_velocity = velocity + DT * force
        return displacement + DT * new_velocity, new_velocity, en[0, :1]

    in_specs = (
        P("ens", "slab", None, None),
        P("ens", "slab", None, None),
        P("ens", "slab", None, None),
        P(),
        P("ens"),
    )
    out_specs = (P("ens", "slab", None, None), P("ens", "slab", None, None), P("ens"))
    return jax.shard_map(body, mesh=mesh, in_specs=in_specs, out_specs=out_specs, check_vma=False)
```

```python
import functools
import math

import jax
import jax.numpy as jnp
import numpy as np
from jax import lax
from jax.experimental import pallas as pl
from jax.experimental.pallas import tpu as pltpu
from jax.sharding import PartitionSpec as P

DT = 0.125
MESH = pl.DeviceIdType.MESH
F32 = jnp.float32


def offset_list():
    up = []
    for a in range(-3, 4):
        for b in range(-3, 4):
            for c in range(-3, 4):
                if a * a + b * b + c * c <= 9 and (a, b, c) > (0, 0, 0):
                    up.append((a, b, c))
    return up + [(-a, -b, -c) for a, b, c in up]


OFFSETS = offset_list()
NUMBER = {o: k for k, o in enumerate(OFFSETS)}
SLOT = {o: k for k, o in enumerate(sorted(OFFSETS))}


def classes(a):
    found = {}
    for o in sorted(OFFSETS):
        if o[0] == a:
            found.setdefault(a * a + o[1] * o[1] + o[2] * o[2], []).append(o)
    return sorted(found.items())


def layer_bits(a, word):
    return sum(1 << (k % 16) for k, o in enumerate(OFFSETS) if o[0] == a and k // 16 == word)


def tables(ny, nz, words):
    in_y = np.zeros((ny, words), np.int64)
    in_z = np.zeros((nz, words), np.int64)
    plane = np.zeros((4, ny, nz), np.float64)
    y, z = np.arange(ny), np.arange(nz)
    for k, (a, b, c) in enumerate(OFFSETS):
        w, bit = k // 16, 1 << (k % 16)
        ok_y = (0 <= y + b) & (y + b < ny)
        ok_z = (0 <= z + c) & (z + c < nz)
        in_y[:, w] |= bit * ok_y
        in_z[:, w] |= bit * ok_z
        if a >= 0:
            r2 = a * a + b * b + c * c
            plane[a] += math.exp(-r2 / 9.0) * r2 * (ok_y[:, None] & ok_z[None, :])
    in_yz = in_y.T[:, :, None] & in_z.T[:, None, :]
    return in_yz.astype(np.int32), plane.astype(np.float32)


def kernel(
    sx, nx,
    u_hbm, v_hbm, w_hbm, yz_hbm, plane_hbm, moduli_hbm, material_hbm,
    force_hbm, en_ref,
    U, S, HY, W, WS, YZ, Q, SI, CX, RX, AL, SA, SB, V, ACC, HM, E1, FA, VEL, FO, EB, moduli, material,
    local, out_sem, us, ur, fs, fr, ts, tr, gs, gr, xs, xr, es, er,
):
    ens = lax.axis_index("ens")
    slab = lax.axis_index("slab")
    nxs = sx // 2
    px = slab // 2
    par = slab % 2
    step = 1 - 2 * par
    partner = (ens, slab + step)
    ahead = (ens, slab + 2 * step)
    behind = (ens, slab - 2 * step)
    has_ahead = jnp.logical_and(px + step >= 0, px + step < nxs)
    has_behind = jnp.logical_and(px - step >= 0, px - step < nxs)
    own_x = U.shape[0] // 3
    ny, nz = U.shape[2:]

    def slab_at(d, other):
        return 2 * ((px + d) % nxs) + (1 - par if other else par)

    def at_x(d):
        return (ens, slab_at(d, False))

    barrier = pltpu.get_barrier_semaphore()
    pl.semaphore_signal(barrier, inc=1, device_id=partner, device_id_type=MESH)
    for d in range(1, nxs):
        pl.semaphore_signal(barrier, inc=1, device_id=at_x(d), device_id_type=MESH)

    def layer(i):
        return i + par * (own_x - 1 - 2 * i)

    loads = []

    def load(src, dst):
        c = pltpu.make_async_copy(src, dst, local.at[len(loads)])
        c.start()
        loads.append(c)
        return c

    u_loads = [load(u_hbm.at[:, layer(i)], U.at[own_x + i]) for i in range(own_x)]
    w_loads = [load(w_hbm.at[:, layer(i)], W.at[i]) for i in range(own_x)]
    w_loads.append(load(yz_hbm, YZ))
    q_loads = [load(plane_hbm, Q), load(moduli_hbm, moduli), load(material_hbm, material)]
    v_loads = [load(v_hbm.at[:, layer(i)], VEL.at[i]) for i in range(own_x)]

    def remote(src, dst, send, recv, dev):
        return pltpu.make_async_remote_copy(
            src_ref=src, dst_ref=dst, send_sem=send, recv_sem=recv, device_id=dev, device_id_type=MESH
        )

    def to_partner(ref, send, recv, i):
        return remote(ref.at[own_x + i], ref.at[3 * own_x - 1 - i], send.at[i], recv.at[i], partner)

    def to_ahead(ref, send, recv, i):
        return remote(ref.at[3 * own_x - 1 - i], ref.at[own_x - 1 - i], send.at[i], recv.at[i], ahead)

    for L in range(own_x):

        @pl.when(jnp.logical_not(has_behind))
        def _():
            RX[L] = jnp.zeros((ny, nz), F32)

        @pl.when(jnp.logical_not(has_ahead))
        def _():
            RX[2 * own_x + L] = jnp.zeros((ny, nz), F32)

    for c in u_loads:
        c.wait()
    pl.semaphore_wait(barrier, nxs)
    rank = (ens // 2) % 8
    turn = jnp.where(rank > 4, 1 + rank % 2, 0)

    def send_u(now):
        @pl.when(turn == now)
        def _():
            for i in range(own_x):
                to_partner(U, us, ur, i).start()

    send_u(0)
    sign = step.astype(F32)
    zero = jnp.zeros((8, nz), F32)

    def clear(L, _):
        for c in range(7):
            for comp in range(3):
                S[c, L, comp, 0:8] = zero
                S[c, L, comp, 8 + ny : 16 + ny] = zero
            for ref in (SA, SB):
                ref[c, L, 0:8] = zero
                ref[c, L, 8 + ny : 16 + ny] = zero
        return 0

    lax.fori_loop(0, 3 * own_x, clear, 0)

    @pl.when(jnp.logical_not(has_behind))
    def _():
        for L in range(own_x):
            for comp in range(3):
                U[L, comp] = jnp.zeros((ny, nz), F32)
            SI[L] = jnp.zeros((ny, nz), F32)

    def rolled(x, c):
        return x if c == 0 else pltpu.roll(x, (-c) % nz, 1)

    def shift_u(L, reach):
        ux = U[L, 0] * sign
        uy = U[L, 1]
        uz = U[L, 2]
        for c in range(-reach, reach + 1):
            S[c + 3, L, 0, 8 : 8 + ny] = rolled(ux, c)
            S[c + 3, L, 1, 8 : 8 + ny] = rolled(uy, c)
            S[c + 3, L, 2, 8 : 8 + ny] = rolled(uz, c) + float(c)

    def shift_to(ref, L, x, reach):
        for c in range(-reach, reach + 1):
            ref[c + 3, L, 8 : 8 + ny] = rolled(x, c)

    def prepare(i, _):
        shift_u(own_x + i, 3)
        uy = U[own_x + i, 1]
        for b in range(-3, 4):
            HY[b + 3, i] = uy - float(b)
        for n in range(3):
            ACC[n, i] = jnp.zeros((ny, nz), F32)
            FA[n, i] = jnp.zeros((ny, nz), F32)
        return 0

    lax.fori_loop(0, own_x, prepare, 0)
    for c in w_loads:
        c.wait()
    base = own_x * slab

    def clean(i, _):
        x = base + layer(i)
        gone = {a: jnp.logical_or(x + a < 0, x + a >= nx).astype(jnp.int32) for a in range(-3, 4) if a}
        for n in range(W.shape[1]):
            keep = 0xFFFF
            for a, out in gone.items():
                if layer_bits(a, n):
                    keep = keep - out * layer_bits(a, n)
            word = W[i, n] & YZ[n] & keep
            W[i, n] = word
            for c in range(-2, 3):
                WS[c + 2, i, n, 0:8] = jnp.zeros((8, nz), jnp.int32)
                WS[c + 2, i, n, 8 + ny : 16 + ny] = jnp.zeros((8, nz), jnp.int32)
                WS[c + 2, i, n, 8 : 8 + ny] = rolled(word, c)
        return 0

    lax.fori_loop(0, own_x, clean, 0)

    def bond(a, b, c, i, L, hx, hz):
        rows = slice(8 + b, 8 + b + ny)
        bx = S[c + 3, L, 0, rows] - hx
        by = S[c + 3, L, 1, rows] - HY[b + 3, i]
        bz = S[c + 3, L, 2, rows] - hz
        return bx, by, bz

    def where_bit(a, b, c):
        kp, km = NUMBER[(a, b, c)], NUMBER[(-a, b, c)]
        word = kp // 16 + par * (km // 16 - kp // 16)
        bit = (1 << (kp % 16)) + par * ((1 << (km % 16)) - (1 << (kp % 16)))
        return word, bit

    def across(a, i):
        L = own_x + i + a
        hx = U[L, 0] * sign + float(a)
        hy = U[L, 1]
        hz = U[L, 2]
        total = None
        for r2, offs in classes(a):
            r, wt = math.sqrt(r2), math.exp(-r2 / 9.0)
            s1 = None
            for _, b, c in offs:
                rows = slice(8 - b, 8 - b + ny)
                bx = S[3 - c, own_x + i, 0, rows] - hx
                by = S[3 - c, own_x + i, 1, rows] - (hy + float(b))
                bz = S[3 - c, own_x + i, 2, rows] - hz
                sq = bx * bx + by * by + bz * bz
                st = sq * lax.rsqrt(sq) - r
                word, bit = where_bit(a, b, c)
                live = (WS[2 - c, i, word, rows] & bit) != 0
                ms = jnp.where(live, st, 0.0)
                s1 = ms if s1 is None else s1 + ms
            total = (wt * r) * s1 if total is None else total + (wt * r) * s1
        return total

    def first(a, i):
        L = own_x + i + a
        hx = U[own_x + i, 0] * sign - float(a)
        hz = U[own_x + i, 2]
        total = [jnp.zeros((ny, nz), F32)] * 3
        for r2, offs in classes(a):
            r, wt = math.sqrt(r2), math.exp(-r2 / 9.0)
            s1 = s2 = s0 = None
            for _, b, c in offs:
                bx, by, bz = bond(a, b, c, i, L, hx, hz)
                sq = bx * bx + by * by + bz * bz
                inv = lax.rsqrt(sq)
                st = sq * inv - r
                word, bit = where_bit(a, b, c)
                live = (W[i, word] & bit) != 0
                ms = jnp.where(live, st, 0.0)
                hm = jnp.where(live, inv, 0.0)
                one = jnp.where(live, 1.0, 0.0)
                HM[SLOT[(a, b, c)], i] = hm * r
                E1[SLOT[(a, b, c)], i] = ms * hm
                s1 = ms if s1 is None else s1 + ms
                s2 = ms * ms if s2 is None else s2 + ms * ms
                s0 = one if s0 is None else s0 + one
            total = [total[0] + (wt * r) * s1, total[1] + wt * s2, total[2] + (wt * r2) * s0]
        for n in range(3):
            ACC[n, i] += total[n]

    def second(a, i):
        L = own_x + i + a
        hx = U[own_x + i, 0] * sign - float(a)
        hz = U[own_x + i, 2]
        ah = AL[own_x + i]
        bh = SB[3, own_x + i, 8 : 8 + ny]
        total = [jnp.zeros((ny, nz), F32)] * 3
        for r2, offs in classes(a):
            wt = math.exp(-r2 / 9.0)
            f = [None] * 3
            for _, b, c in offs:
                rows = slice(8 + b, 8 + b + ny)
                k = SLOT[(a, b, c)]
                t = (bh + SB[c + 3, L, rows]) * E1[k, i] + (ah + SA[c + 3, L, rows]) * HM[k, i]
                y = bond(a, b, c, i, L, hx, hz)
                f = [t * y[n] if f[n] is None else f[n] + t * y[n] for n in range(3)]
            total = [total[n] + wt * f[n] for n in range(3)]
        for n in range(3):
            FA[n, i] += total[n]

    def inner(block):
        def at(a, lo, hi):
            def one(i, _):
                block(a, i)
                return 0

            lax.fori_loop(lo, hi, one, 0)

        for a in range(-2, 3):
            at(a, max(0, -a), own_x - max(0, a))

    def outer(block, L):
        for i in range(own_x):
            a = L - own_x - i
            if -3 <= a <= 3:
                block(a, i)

    send_u(1)
    inner(first)
    send_u(2)
    for i in range(own_x):
        SI[own_x + i] = ACC[0, i]

    for c in q_loads:
        c.wait()
    bulk = moduli[0, material[0]]
    shear = moduli[1, material[0]]
    factor = 3.0 * bulk - 5.0 * shear

    def volumes(L, _):
        x = base + layer(L - own_x)
        sums = jnp.zeros((ny, nz), F32)
        for a in range(4):
            up = jnp.logical_and(x + a >= 0, x + a < nx).astype(F32)
            down = jnp.logical_and(x - a >= 0, x - a < nx).astype(F32)
            sums = sums + (up if a == 0 else up + down) * Q[a]
        home = jnp.logical_and(x >= 0, x < nx)
        vol = jnp.where(home, sums, 1.0)
        V[L] = vol
        shift_to(SB, L, 15.0 * shear / vol, 3)
        return 0

    lax.fori_loop(0, own_x, volumes, 0)
    for i in range(own_x):
        to_partner(SI, ts, tr, i).start()
    lax.fori_loop(own_x, 3 * own_x, volumes, 0)

    def arrived(L):
        shift_u(L, 2)
        outer(first, L)
        total = None
        for i in range(own_x):
            a = L - own_x - i
            if -3 <= a <= 3:
                part = across(a, i)
                total = part if total is None else total + part
        CX[L] = total

    for i in range(own_x):
        to_partner(U, us, ur, i).wait_recv()

        @pl.when(has_ahead)
        def _():
            to_ahead(U, fs, fr, i).start()

        arrived(3 * own_x - 1 - i)

    n = own_x
    part_up = remote(CX.at[pl.ds(2 * n, n)], RX.at[pl.ds(0, n)], xs.at[0], xr.at[0], ahead)
    part_down = remote(CX.at[pl.ds(0, n)], RX.at[pl.ds(2 * n, n)], xs.at[1], xr.at[1], behind)

    @pl.when(has_ahead)
    def _():
        part_up.start()

    for i in range(own_x):

        @pl.when(has_behind)
        def _():
            to_ahead(U, fs, fr, i).wait_recv()

        arrived(own_x - 1 - i)

    def dilate(i, _):
        vol = V[own_x + i]
        a = factor * (3.0 * ACC[0, i] / vol) / vol
        AL[own_x + i] = a
        shift_to(SA, own_x + i, a, 3)
        return 0

    lax.fori_loop(0, own_x, dilate, 0)

    @pl.when(has_behind)
    def _():
        part_down.start()

    for i in range(own_x):
        to_partner(SI, ts, tr, i).wait_recv()

        @pl.when(has_ahead)
        def _():
            to_ahead(SI, gs, gr, i).start()

    inner(second)

    def halo(L):
        vol = V[L]
        shift_to(SA, L, factor * (3.0 * (SI[L] + CX[L] + RX[L]) / vol) / vol, 2)
        outer(second, L)

    @pl.when(has_ahead)
    def _():
        part_down.wait_recv()

    for i in range(own_x):
        halo(3 * own_x - 1 - i)

    @pl.when(has_behind)
    def _():
        part_up.wait_recv()

    for i in range(own_x):

        @pl.when(has_behind)
        def _():
            to_ahead(SI, gs, gr, i).wait_recv()

        halo(own_x - 1 - i)

    for c in v_loads:
        c.wait()
    heat = jnp.zeros((ny, nz), F32)
    for i in range(own_x):
        kinetic = None
        for n in range(3):
            force = FA[n, i] * sign if n == 0 else FA[n, i]
            FO[i, n] = force
            nv = VEL[i, n] + DT * force
            kinetic = nv * nv if kinetic is None else kinetic + nv * nv
        vol = V[own_x + i]
        th = 3.0 * ACC[0, i] / vol
        th2 = th * th
        strain = ACC[1, i] - (2.0 / 9.0) * th2 * vol + th2 * ACC[2, i] * (1.0 / 9.0)
        heat = heat + 0.5 * kinetic + 0.5 * bulk * th2 + 7.5 * shear * strain / vol
    EB[slab] = jnp.sum(heat, axis=0, keepdims=True)

    outs = []
    for i in range(own_x):
        c = pltpu.make_async_copy(FO.at[i], force_hbm.at[:, layer(i)], out_sem.at[i])
        c.start()
        outs.append(c)

    peers = [(d, o) for o in (True, False) for d in range(nxs) if d or o]
    rows = []
    for n, (d, o) in enumerate(peers):
        c = remote(EB.at[slab], EB.at[slab], es.at[n], er.at[slab], (ens, slab_at(d, o)))
        c.start()
        rows.append(c)
    for c in outs:
        c.wait()
    for i in range(own_x):
        to_partner(U, us, ur, i).wait_send()
        to_partner(SI, ts, tr, i).wait_send()

        @pl.when(has_ahead)
        def _():
            to_ahead(U, fs, fr, i).wait_send()
            to_ahead(SI, gs, gr, i).wait_send()

    @pl.when(has_ahead)
    def _():
        part_up.wait_send()

    @pl.when(has_behind)
    def _():
        part_down.wait_send()

    for c in rows:
        c.wait_send()
    for n, (d, o) in enumerate(peers):
        q = slab_at(d, o)
        remote(EB.at[q], EB.at[q], es.at[n], er.at[q], (ens, q)).wait_recv()
    whole = EB[0]
    for n in range(1, sx):
        whole = whole + EB[n]
    en_ref[...] = whole


def finish(cells, force, heat, displacement, velocity, nu, nv, energy):
    moved = velocity[...] + DT * force[...]
    nv[...] = moved
    nu[...] = displacement[...] + DT * moved
    energy[0] = jnp.sum(heat[...]) * (1.0 / cells)


def solution(mesh):
    slabs = mesh.shape["slab"]

    def body(displacement, velocity, bond_mask, moduli, material):
        own_x, ny, nz = displacement.shape[1:]
        words = bond_mask.shape[0]
        nx = own_x * slabs
        in_yz, plane = tables(ny, nz, words)
        grid = (ny, nz)
        tall = (ny + 16, nz)
        nb = len(OFFSETS)
        vm = pltpu.VMEM
        dma = pltpu.SemaphoreType.DMA
        hbm = pl.BlockSpec(memory_space=pltpu.HBM)
        vmem = pl.BlockSpec(memory_space=pltpu.VMEM)
        force, en = pl.pallas_call(
            functools.partial(kernel, slabs, nx),
            out_shape=(jax.ShapeDtypeStruct(displacement.shape, F32), jax.ShapeDtypeStruct((1, nz), F32)),
            in_specs=[hbm] * 7,
            out_specs=(hbm, vmem),
            scratch_shapes=[
                vm((3 * own_x, 3) + grid, F32),
                vm((7, 3 * own_x, 3) + tall, F32),
                vm((7, own_x) + grid, F32),
                vm((own_x, words) + grid, jnp.int32),
                vm((5, own_x, words) + tall, jnp.int32),
                vm((words,) + grid, jnp.int32),
                vm((4,) + grid, F32),
                vm((3 * own_x,) + grid, F32),
                vm((3 * own_x,) + grid, F32),
                vm((3 * own_x,) + grid, F32),
                vm((3 * own_x,) + grid, F32),
                vm((7, 3 * own_x) + tall, F32),
                vm((7, 3 * own_x) + tall, F32),
                vm((3 * own_x,) + grid, F32),
                vm((3, own_x) + grid, F32),
                vm((nb, own_x) + grid, F32),
                vm((nb, own_x) + grid, F32),
                vm((3, own_x) + grid, F32),
                vm((own_x, 3) + grid, F32),
                vm((own_x, 3) + grid, F32),
                vm((slabs, 1, nz), F32),
                pltpu.SMEM(moduli.shape[::-1], F32),
                pltpu.SMEM(material.shape, jnp.int32),
                dma((3 * own_x + 4,)),
                dma((own_x,)),
                dma((own_x,)), dma((own_x,)), dma((own_x,)), dma((own_x,)),
                dma((own_x,)), dma((own_x,)), dma((own_x,)), dma((own_x,)),
                dma((2,)), dma((2,)),
                dma((slabs,)), dma((slabs,)),
            ],
            compiler_params=pltpu.CompilerParams(collective_id=0, has_side_effects=True),
        )(
            displacement, velocity, bond_mask, jnp.asarray(in_yz), jnp.asarray(plane),
            moduli.T, material,
        )
        full = jax.ShapeDtypeStruct(displacement.shape, F32)
        return pl.pallas_call(
            functools.partial(finish, nx * ny * nz),
            out_shape=(full, full, jax.ShapeDtypeStruct((1,), F32)),
            in_specs=[vmem] * 4,
            out_specs=(vmem, vmem, pl.BlockSpec(memory_space=pltpu.SMEM)),
        )(force, en, displacement, velocity)

    in_specs = (
        P("ens", "slab", None, None),
        P("ens", "slab", None, None),
        P("ens", "slab", None, None),
        P(),
        P("ens"),
    )
    out_specs = (P("ens", "slab", None, None), P("ens", "slab", None, None), P("ens"))
    return jax.shard_map(body, mesh=mesh, in_specs=in_specs, out_specs=out_specs, check_vma=False)
```

```python
import functools
import math

import jax
import jax.numpy as jnp
import numpy as np
from jax import lax
from jax.experimental import pallas as pl
from jax.experimental.pallas import tpu as pltpu
from jax.sharding import PartitionSpec as P

DT = 0.125
MESH = pl.DeviceIdType.MESH
F32 = jnp.float32


def offset_list():
    up = []
    for a in range(-3, 4):
        for b in range(-3, 4):
            for c in range(-3, 4):
                if a * a + b * b + c * c <= 9 and (a, b, c) > (0, 0, 0):
                    up.append((a, b, c))
    return up + [(-a, -b, -c) for a, b, c in up]


OFFSETS = offset_list()
NUMBER = {o: k for k, o in enumerate(OFFSETS)}
SLOT = {o: k for k, o in enumerate(sorted(OFFSETS))}


def classes(a):
    found = {}
    for o in sorted(OFFSETS):
        if o[0] == a:
            found.setdefault(a * a + o[1] * o[1] + o[2] * o[2], []).append(o)
    return sorted(found.items())


def layer_bits(a, word):
    return sum(1 << (k % 16) for k, o in enumerate(OFFSETS) if o[0] == a and k // 16 == word)


def tables(ny, nz, words):
    in_y = np.zeros((ny, words), np.int64)
    in_z = np.zeros((nz, words), np.int64)
    plane = np.zeros((4, ny, nz), np.float64)
    y, z = np.arange(ny), np.arange(nz)
    for k, (a, b, c) in enumerate(OFFSETS):
        w, bit = k // 16, 1 << (k % 16)
        ok_y = (0 <= y + b) & (y + b < ny)
        ok_z = (0 <= z + c) & (z + c < nz)
        in_y[:, w] |= bit * ok_y
        in_z[:, w] |= bit * ok_z
        if a >= 0:
            r2 = a * a + b * b + c * c
            plane[a] += math.exp(-r2 / 9.0) * r2 * (ok_y[:, None] & ok_z[None, :])
    in_yz = in_y.T[:, :, None] & in_z.T[:, None, :]
    return in_yz.astype(np.int32), plane.astype(np.float32)


def kernel(
    sx, nx,
    u_hbm, v_hbm, w_hbm, yz_hbm, plane_hbm, moduli_hbm, material_hbm,
    force_hbm, en_ref,
    U, S, HY, W, WS, YZ, Q, SI, CX, RX, AL, SA, SB, V, ACC, HM, E1, FA, VEL, FO, EB, moduli, material,
    local, out_sem, us, ur, fs, fr, ts, tr, gs, gr, xs, xr, es, er,
):
    ens = lax.axis_index("ens")
    slab = lax.axis_index("slab")
    nxs = sx // 2
    px = slab // 2
    par = slab % 2
    step = 1 - 2 * par
    partner = (ens, slab + step)
    ahead = (ens, slab + 2 * step)
    behind = (ens, slab - 2 * step)
    has_ahead = jnp.logical_and(px + step >= 0, px + step < nxs)
    has_behind = jnp.logical_and(px - step >= 0, px - step < nxs)
    own_x = U.shape[0] // 3
    ny, nz = U.shape[2:]

    def slab_at(d, other):
        return 2 * ((px + d) % nxs) + (1 - par if other else par)

    def at_x(d):
        return (ens, slab_at(d, False))

    barrier = pltpu.get_barrier_semaphore()
    pl.semaphore_signal(barrier, inc=1, device_id=partner, device_id_type=MESH)
    for d in range(1, nxs):
        pl.semaphore_signal(barrier, inc=1, device_id=at_x(d), device_id_type=MESH)

    def layer(i):
        return i + par * (own_x - 1 - 2 * i)

    loads = []

    def load(src, dst):
        c = pltpu.make_async_copy(src, dst, local.at[len(loads)])
        c.start()
        loads.append(c)
        return c

    u_loads = [load(u_hbm.at[:, layer(i)], U.at[own_x + i]) for i in range(own_x)]
    w_loads = [load(w_hbm.at[:, layer(i)], W.at[i]) for i in range(own_x)]
    w_loads.append(load(yz_hbm, YZ))
    q_loads = [load(plane_hbm, Q), load(moduli_hbm, moduli), load(material_hbm, material)]
    v_load = load(v_hbm, VEL)

    def remote(src, dst, send, recv, dev):
        return pltpu.make_async_remote_copy(
            src_ref=src, dst_ref=dst, send_sem=send, recv_sem=recv, device_id=dev, device_id_type=MESH
        )

    def to_partner(ref, send, recv, i):
        return remote(ref.at[own_x + i], ref.at[3 * own_x - 1 - i], send.at[i], recv.at[i], partner)

    def to_ahead(ref, send, recv, i):
        return remote(ref.at[3 * own_x - 1 - i], ref.at[own_x - 1 - i], send.at[i], recv.at[i], ahead)

    for L in range(own_x):

        @pl.when(jnp.logical_not(has_behind))
        def _():
            RX[L] = jnp.zeros((ny, nz), F32)

        @pl.when(jnp.logical_not(has_ahead))
        def _():
            RX[2 * own_x + L] = jnp.zeros((ny, nz), F32)

    for c in u_loads:
        c.wait()
    pl.semaphore_wait(barrier, nxs)
    rank = (ens // 2) % 8
    turn = jnp.where(rank > 4, 1 + rank // 7, 0)

    def send_u(now):
        @pl.when(turn == now)
        def _():
            for i in range(own_x):
                to_partner(U, us, ur, i).start()

    send_u(0)
    sign = step.astype(F32)
    zero = jnp.zeros((8, nz), F32)

    def clear(L, _):
        for c in range(7):
            for comp in range(3):
                S[c, L, comp, 0:8] = zero
                S[c, L, comp, 8 + ny : 16 + ny] = zero
            for ref in (SA, SB):
                ref[c, L, 0:8] = zero
                ref[c, L, 8 + ny : 16 + ny] = zero
        return 0

    lax.fori_loop(0, 3 * own_x, clear, 0)

    @pl.when(jnp.logical_not(has_behind))
    def _():
        for L in range(own_x):
            for comp in range(3):
                U[L, comp] = jnp.zeros((ny, nz), F32)
            SI[L] = jnp.zeros((ny, nz), F32)

    def rolled(x, c):
        return x if c == 0 else pltpu.roll(x, (-c) % nz, 1)

    def shift_u(L, reach):
        ux = U[L, 0] * sign
        uy = U[L, 1]
        uz = U[L, 2]
        for c in range(-reach, reach + 1):
            S[c + 3, L, 0, 8 : 8 + ny] = rolled(ux, c)
            S[c + 3, L, 1, 8 : 8 + ny] = rolled(uy, c)
            S[c + 3, L, 2, 8 : 8 + ny] = rolled(uz, c) + float(c)

    def shift_to(ref, L, x, reach):
        for c in range(-reach, reach + 1):
            ref[c + 3, L, 8 : 8 + ny] = rolled(x, c)

    def prepare(i, _):
        shift_u(own_x + i, 3)
        uy = U[own_x + i, 1]
        for b in range(-3, 4):
            HY[b + 3, i] = uy - float(b)
        for n in range(3):
            ACC[n, i] = jnp.zeros((ny, nz), F32)
            FA[n, i] = jnp.zeros((ny, nz), F32)
        return 0

    lax.fori_loop(0, own_x, prepare, 0)
    for c in w_loads:
        c.wait()
    base = own_x * slab

    def clean(i, _):
        x = base + layer(i)
        gone = {a: jnp.logical_or(x + a < 0, x + a >= nx).astype(jnp.int32) for a in range(-3, 4) if a}
        for n in range(W.shape[1]):
            keep = 0xFFFF
            for a, out in gone.items():
                if layer_bits(a, n):
                    keep = keep - out * layer_bits(a, n)
            word = W[i, n] & YZ[n] & keep
            W[i, n] = word
            for c in range(-2, 3):
                WS[c + 2, i, n, 0:8] = jnp.zeros((8, nz), jnp.int32)
                WS[c + 2, i, n, 8 + ny : 16 + ny] = jnp.zeros((8, nz), jnp.int32)
                WS[c + 2, i, n, 8 : 8 + ny] = rolled(word, c)
        return 0

    lax.fori_loop(0, own_x, clean, 0)

    def bond(a, b, c, i, L, hx, hz):
        rows = slice(8 + b, 8 + b + ny)
        bx = S[c + 3, L, 0, rows] - hx
        by = S[c + 3, L, 1, rows] - HY[b + 3, i]
        bz = S[c + 3, L, 2, rows] - hz
        return bx, by, bz

    def where_bit(a, b, c):
        kp, km = NUMBER[(a, b, c)], NUMBER[(-a, b, c)]
        word = kp // 16 + par * (km // 16 - kp // 16)
        bit = (1 << (kp % 16)) + par * ((1 << (km % 16)) - (1 << (kp % 16)))
        return word, bit

    def across(a, i):
        L = own_x + i + a
        hx = U[L, 0] * sign + float(a)
        hy = U[L, 1]
        hz = U[L, 2]
        total = None
        for r2, offs in classes(a):
            r, wt = math.sqrt(r2), math.exp(-r2 / 9.0)
            s1 = None
            for _, b, c in offs:
                rows = slice(8 - b, 8 - b + ny)
                bx = S[3 - c, own_x + i, 0, rows] - hx
                by = S[3 - c, own_x + i, 1, rows] - (hy + float(b))
                bz = S[3 - c, own_x + i, 2, rows] - hz
                sq = bx * bx + by * by + bz * bz
                st = sq * lax.rsqrt(sq) - r
                word, bit = where_bit(a, b, c)
                live = (WS[2 - c, i, word, rows] & bit) != 0
                ms = jnp.where(live, st, 0.0)
                s1 = ms if s1 is None else s1 + ms
            total = (wt * r) * s1 if total is None else total + (wt * r) * s1
        return total

    def first(a, i):
        L = own_x + i + a
        hx = U[own_x + i, 0] * sign - float(a)
        hz = U[own_x + i, 2]
        total = [jnp.zeros((ny, nz), F32)] * 3
        for r2, offs in classes(a):
            r, wt = math.sqrt(r2), math.exp(-r2 / 9.0)
            s1 = s2 = s0 = None
            for _, b, c in offs:
                bx, by, bz = bond(a, b, c, i, L, hx, hz)
                sq = bx * bx + by * by + bz * bz
                inv = lax.rsqrt(sq)
                st = sq * inv - r
                word, bit = where_bit(a, b, c)
                live = (W[i, word] & bit) != 0
                ms = jnp.where(live, st, 0.0)
                hm = jnp.where(live, inv, 0.0)
                one = jnp.where(live, 1.0, 0.0)
                HM[SLOT[(a, b, c)], i] = hm * r
                E1[SLOT[(a, b, c)], i] = ms * hm
                s1 = ms if s1 is None else s1 + ms
                s2 = ms * ms if s2 is None else s2 + ms * ms
                s0 = one if s0 is None else s0 + one
            total = [total[0] + (wt * r) * s1, total[1] + wt * s2, total[2] + (wt * r2) * s0]
        for n in range(3):
            ACC[n, i] += total[n]

    def second(a, i):
        L = own_x + i + a
        hx = U[own_x + i, 0] * sign - float(a)
        hz = U[own_x + i, 2]
        ah = AL[own_x + i]
        bh = SB[3, own_x + i, 8 : 8 + ny]
        total = [jnp.zeros((ny, nz), F32)] * 3
        for r2, offs in classes(a):
            wt = math.exp(-r2 / 9.0)
            f = [None] * 3
            for _, b, c in offs:
                rows = slice(8 + b, 8 + b + ny)
                k = SLOT[(a, b, c)]
                t = (bh + SB[c + 3, L, rows]) * E1[k, i] + (ah + SA[c + 3, L, rows]) * HM[k, i]
                y = bond(a, b, c, i, L, hx, hz)
                f = [t * y[n] if f[n] is None else f[n] + t * y[n] for n in range(3)]
            total = [total[n] + wt * f[n] for n in range(3)]
        for n in range(3):
            FA[n, i] += total[n]

    def inner(block):
        def at(a, lo, hi):
            def one(i, _):
                block(a, i)
                return 0

            lax.fori_loop(lo, hi, one, 0)

        for a in range(-2, 3):
            at(a, max(0, -a), own_x - max(0, a))

    def outer(block, L):
        for i in range(own_x):
            a = L - own_x - i
            if -3 <= a <= 3:
                block(a, i)

    send_u(1)
    inner(first)
    send_u(2)
    for i in range(own_x):
        SI[2 * own_x - 1 - i] = ACC[0, i]

    for c in q_loads:
        c.wait()
    bulk = moduli[0, material[0]]
    shear = moduli[1, material[0]]
    factor = 3.0 * bulk - 5.0 * shear

    def volumes(L, _):
        x = base + layer(L - own_x)
        sums = jnp.zeros((ny, nz), F32)
        for a in range(4):
            up = jnp.logical_and(x + a >= 0, x + a < nx).astype(F32)
            down = jnp.logical_and(x - a >= 0, x - a < nx).astype(F32)
            sums = sums + (up if a == 0 else up + down) * Q[a]
        home = jnp.logical_and(x >= 0, x < nx)
        vol = jnp.where(home, sums, 1.0)
        V[L] = vol
        shift_to(SB, L, 15.0 * shear / vol, 3)
        return 0

    lax.fori_loop(0, own_x, volumes, 0)
    n = own_x
    sums_over = remote(SI.at[pl.ds(n, n)], SI.at[pl.ds(2 * n, n)], ts, tr, partner)
    sums_on = remote(SI.at[pl.ds(2 * n, n)], SI.at[pl.ds(0, n)], gs, gr, ahead)
    sums_over.start()
    lax.fori_loop(own_x, 3 * own_x, volumes, 0)

    def arrived(L):
        shift_u(L, 2)
        outer(first, L)
        total = None
        for i in range(own_x):
            a = L - own_x - i
            if -3 <= a <= 3:
                part = across(a, i)
                total = part if total is None else total + part
        CX[L] = total

    for i in range(own_x):
        to_partner(U, us, ur, i).wait_recv()

        @pl.when(has_ahead)
        def _():
            to_ahead(U, fs, fr, i).start()

        arrived(3 * own_x - 1 - i)

    part_up = remote(CX.at[pl.ds(2 * n, n)], RX.at[pl.ds(0, n)], xs.at[0], xr.at[0], ahead)
    part_down = remote(CX.at[pl.ds(0, n)], RX.at[pl.ds(2 * n, n)], xs.at[1], xr.at[1], behind)

    @pl.when(has_ahead)
    def _():
        part_up.start()

    for i in range(own_x):

        @pl.when(has_behind)
        def _():
            to_ahead(U, fs, fr, i).wait_recv()

        arrived(own_x - 1 - i)

    def dilate(i, _):
        vol = V[own_x + i]
        a = factor * (3.0 * ACC[0, i] / vol) / vol
        AL[own_x + i] = a
        shift_to(SA, own_x + i, a, 3)
        return 0

    lax.fori_loop(0, own_x, dilate, 0)

    @pl.when(has_behind)
    def _():
        part_down.start()

    sums_over.wait_recv()

    @pl.when(has_ahead)
    def _():
        sums_on.start()

    inner(second)

    def halo(L):
        vol = V[L]
        shift_to(SA, L, factor * (3.0 * (SI[L] + CX[L] + RX[L]) / vol) / vol, 2)
        outer(second, L)

    @pl.when(has_ahead)
    def _():
        part_down.wait_recv()

    for i in range(own_x):
        halo(3 * own_x - 1 - i)

    @pl.when(has_behind)
    def _():
        part_up.wait_recv()

    @pl.when(has_behind)
    def _():
        sums_on.wait_recv()

    for i in range(own_x):
        halo(own_x - 1 - i)

    v_load.wait()
    heat = jnp.zeros((ny, nz), F32)
    for i in range(own_x):
        kinetic = None
        for n in range(3):
            force = FA[n, i] * sign if n == 0 else FA[n, i]
            FO[n, layer(i)] = force
            nv = VEL[n, layer(i)] + DT * force
            kinetic = nv * nv if kinetic is None else kinetic + nv * nv
        vol = V[own_x + i]
        th = 3.0 * ACC[0, i] / vol
        th2 = th * th
        strain = ACC[1, i] - (2.0 / 9.0) * th2 * vol + th2 * ACC[2, i] * (1.0 / 9.0)
        heat = heat + 0.5 * kinetic + 0.5 * bulk * th2 + 7.5 * shear * strain / vol
    EB[slab] = jnp.sum(heat, axis=0, keepdims=True)

    out = pltpu.make_async_copy(FO, force_hbm, out_sem)
    out.start()

    peers = [(d, o) for o in (True, False) for d in range(nxs) if d or o]
    rows = []
    for n, (d, o) in enumerate(peers):
        c = remote(EB.at[slab], EB.at[slab], es.at[n], er.at[slab], (ens, slab_at(d, o)))
        c.start()
        rows.append(c)
    out.wait()
    for i in range(own_x):
        to_partner(U, us, ur, i).wait_send()

        @pl.when(has_ahead)
        def _():
            to_ahead(U, fs, fr, i).wait_send()

    sums_over.wait_send()

    @pl.when(has_ahead)
    def _():
        part_up.wait_send()
        sums_on.wait_send()

    @pl.when(has_behind)
    def _():
        part_down.wait_send()

    for c in rows:
        c.wait_send()
    for n, (d, o) in enumerate(peers):
        q = slab_at(d, o)
        remote(EB.at[q], EB.at[q], es.at[n], er.at[q], (ens, q)).wait_recv()
    whole = EB[0]
    for n in range(1, sx):
        whole = whole + EB[n]
    en_ref[...] = whole


def finish(cells, force, heat, displacement, velocity, nu, nv, energy):
    moved = velocity[...] + DT * force[...]
    nv[...] = moved
    nu[...] = displacement[...] + DT * moved
    energy[0] = jnp.sum(heat[...]) * (1.0 / cells)


def solution(mesh):
    slabs = mesh.shape["slab"]

    def body(displacement, velocity, bond_mask, moduli, material):
        own_x, ny, nz = displacement.shape[1:]
        words = bond_mask.shape[0]
        nx = own_x * slabs
        in_yz, plane = tables(ny, nz, words)
        grid = (ny, nz)
        tall = (ny + 16, nz)
        nb = len(OFFSETS)
        vm = pltpu.VMEM
        dma = pltpu.SemaphoreType.DMA
        hbm = pl.BlockSpec(memory_space=pltpu.HBM)
        vmem = pl.BlockSpec(memory_space=pltpu.VMEM)
        force, en = pl.pallas_call(
            functools.partial(kernel, slabs, nx),
            out_shape=(jax.ShapeDtypeStruct(displacement.shape, F32), jax.ShapeDtypeStruct((1, nz), F32)),
            in_specs=[hbm] * 7,
            out_specs=(hbm, vmem),
            scratch_shapes=[
                vm((3 * own_x, 3) + grid, F32),
                vm((7, 3 * own_x, 3) + tall, F32),
                vm((7, own_x) + grid, F32),
                vm((own_x, words) + grid, jnp.int32),
                vm((5, own_x, words) + tall, jnp.int32),
                vm((words,) + grid, jnp.int32),
                vm((4,) + grid, F32),
                vm((3 * own_x,) + grid, F32),
                vm((3 * own_x,) + grid, F32),
                vm((3 * own_x,) + grid, F32),
                vm((3 * own_x,) + grid, F32),
                vm((7, 3 * own_x) + tall, F32),
                vm((7, 3 * own_x) + tall, F32),
                vm((3 * own_x,) + grid, F32),
                vm((3, own_x) + grid, F32),
                vm((nb, own_x) + grid, F32),
                vm((nb, own_x) + grid, F32),
                vm((3, own_x) + grid, F32),
                vm((3, own_x) + grid, F32),
                vm((3, own_x) + grid, F32),
                vm((slabs, 1, nz), F32),
                pltpu.SMEM(moduli.shape[::-1], F32),
                pltpu.SMEM(material.shape, jnp.int32),
                dma((2 * own_x + 5,)),
                dma,
                dma((own_x,)), dma((own_x,)), dma((own_x,)), dma((own_x,)),
                dma, dma, dma, dma,
                dma((2,)), dma((2,)),
                dma((slabs,)), dma((slabs,)),
            ],
            compiler_params=pltpu.CompilerParams(collective_id=0, has_side_effects=True),
        )(
            displacement, velocity, bond_mask, jnp.asarray(in_yz), jnp.asarray(plane),
            moduli.T, material,
        )
        full = jax.ShapeDtypeStruct(displacement.shape, F32)
        return pl.pallas_call(
            functools.partial(finish, nx * ny * nz),
            out_shape=(full, full, jax.ShapeDtypeStruct((1,), F32)),
            in_specs=[vmem] * 4,
            out_specs=(vmem, vmem, pl.BlockSpec(memory_space=pltpu.SMEM)),
        )(force, en, displacement, velocity)

    in_specs = (
        P("ens", "slab", None, None),
        P("ens", "slab", None, None),
        P("ens", "slab", None, None),
        P(),
        P("ens"),
    )
    out_specs = (P("ens", "slab", None, None), P("ens", "slab", None, None), P("ens"))
    return jax.shard_map(body, mesh=mesh, in_specs=in_specs, out_specs=out_specs, check_vma=False)
```
